256 devices in a mesh: tm: 32 (over z, y_hi, core), space: 8 (over x, y_lo).
Axes of the slice: x: 4, y: 4 (y_hi: 2, y_lo: 2; y = y_hi * 2 + y_lo), z: 8, core: 2. Of those that a mesh axis runs over, the one named last changes fastest.
Arguments:
- start_states: float32 [32, 3, 16, 256, 256], P('tm', None, 'space'), may hold values from -6 to 6
- wall_normal: bfloat16 [256, 256], replicated, may hold values from -0.375 to 0.375
- spanwise: bfloat16 [256, 256], replicated, may hold values from -0.375 to 0.375
- base_flow: float32 [3, 256], replicated, may hold values from -1.5 to 1.5
Outputs:
- end_state: float32 [32, 3, 16, 256, 256], P('tm', None, 'space')
The draws below stay inside these ranges and needn't reach their ends.
All inputs are finite; a program needn't handle non-finite values.
Results may differ from the reference program's by a relative error of at most 0.0017.
Values sent between devices are 32-bit elements; how exact they have to be, the bound alone decides.
No kernel may reach another device: no remote copies, remote signals or barrier semaphores. Data moves between devices by JAX's collectives and lax.ppermute only.
A program may use at most 64 MiB of HBM per device.

```python
from functools import partial
import jax
import jax.numpy as jnp
from jax import lax

Y = 256
Z = 256
TICKS = 2
NX = 16
SLICES = 32


def shard_levels(own_key, dims, cuts, smallest, top_value):
    gain, own = 1.0, jax.random.fold_in(own_key, 6)
    for position, parts in cuts:
        heights = jnp.exp(jax.random.uniform(jax.random.fold_in(own, position), (parts,), jnp.float32, smallest / len(cuts), top_value / len(cuts)))
        gain = gain * jnp.repeat(heights, dims[position] // parts).reshape([-1 if axis == position else 1 for axis in range(len(dims))])
    return gain


def bell_draw(key, shape, width, limit, split=(), held_as=jnp.bfloat16):
    level = shard_levels(key, shape, split, -0.22, 0.18) if split else 1.0
    entries = jax.random.normal(key, shape, jnp.float32) * width * level
    return jnp.minimum(jnp.maximum(entries, -limit), limit).astype(held_as)


def setup_inputs(seed: int = 0) -> dict:
    arg_keys = jax.random.split(jax.random.key(seed), 5)
    return {
        "start_states": bell_draw(arg_keys[0], (SLICES, 3, NX, Y, Z), 1.0, 6.0, ((0, 32), (2, 8)), jnp.float32),
        "wall_normal": bell_draw(arg_keys[1], (Y, Y), Y ** -0.5, 0.375),
        "spanwise": bell_draw(arg_keys[2], (Z, Z), Z ** -0.5, 0.375),
        "base_flow": jnp.clip(jax.random.uniform(arg_keys[3], (3, Y), jnp.float32, -1.5, 1.5), -1.5, 1.5),
    }


step_size = 0.2


def tendency(q, wall_normal, spanwise, base_flow):
    grad_x = 0.5 * (jnp.roll(q, -1, axis=1) - jnp.roll(q, 1, axis=1))
    rounded = q.astype(jnp.bfloat16).astype(jnp.float32)
    grad_y = jnp.einsum("yk,cxkz->cxyz", wall_normal.astype(jnp.float32), rounded, precision=lax.Precision.HIGHEST)
    grad_z = jnp.einsum("cxyk,kz->cxyz", rounded, spanwise.astype(jnp.float32), precision=lax.Precision.HIGHEST)
    velocity = base_flow[:, None, :, None] + q
    return -(velocity[0:1] * grad_x + velocity[1:2] * grad_y + velocity[2:3] * grad_z)


def reference(start_states, wall_normal, spanwise, base_flow):
    evaluate = partial(tendency, wall_normal=wall_normal, spanwise=spanwise, base_flow=base_flow)
    begin = start_states
    finish = start_states
    old_rate = lax.map(evaluate, begin)
    fresh = old_rate
    for tick in range(TICKS):
        if tick > 0:
            fresh = lax.map(evaluate, begin)
        end_rate = lax.map(evaluate, finish)
        finish = begin + step_size * (fresh - old_rate) + 0.5 * step_size * (old_rate + end_rate)
        old_rate = fresh
        if tick < TICKS - 1:
            begin = jnp.concatenate([begin[:1], finish[:-1]], axis=0)
    return finish
```

```python
import functools

import jax
import jax.numpy as jnp
from jax import lax
from jax.experimental import pallas as pl
from jax.experimental.pallas import tpu as pltpu
from jax.sharding import PartitionSpec as P

AXES = ("tm", "space")
STEP = 0.2


def routes(slices, slabs):
    at = lambda s, p: s * slabs + p % slabs
    cells = [(k, x, l) for k in range(slices // 2) for x in range(slabs // 2) for l in range(2)]
    side = lambda l: 1 - 2 * l
    stay = lambda k, x, l: at(2 * k + l, 2 * x + l)
    move = lambda k, x, l: at(2 * k + 1 - l, 2 * x + l)
    return {
        "swap": [(move(k, x, l), move(k, x, 1 - l)) for k, x, l in cells],
        "near_in": [(stay(k, x, l), move(k, x, l)) for k, x, l in cells],
        "far_in": [(stay(k, x + side(l), l), move(k, x, l)) for k, x, l in cells],
        "near_out": [(move(k, x, l), stay(k, x, l)) for k, x, l in cells],
        "far_out": [(move(k, x, l), stay(k, x + side(l), l)) for k, x, l in cells],
        "next_move": [
            (move(k, x, l), at(2 * k + l + 1, 2 * x + 1 - l)) for k, x, l in cells if 2 * k + l + 1 < slices
        ],
        "next_stay": [(stay(k, x, l), at(2 * k + l + 1, 2 * x + l)) for k, x, l in cells if 2 * k + l + 1 < slices],
    }


def advance(flags, near, own, far, wall, span, flow, a_ref, b_ref, mid):
    low = flags[0]
    sign = jnp.where(low == 1, 0.5, -0.5).astype(jnp.float32)
    first = jnp.where(flags[1] == 1, 1.0, 0.0).astype(jnp.float32)
    one = lambda i: jnp.where(low == 1, i, 1 - i)
    order = [(near, one(0)), (near, one(1)), (own, one(0)), (own, one(1)), (far, one(0)), (far, one(1))]

    def rate(before, here, after):
        fields = [here(c) for c in range(3)]
        vel = [flow[c] + fields[c] for c in range(3)]
        vx = vel[0] * sign
        out = []
        for c in range(3):
            rounded = fields[c].astype(jnp.bfloat16)
            gy = jnp.dot(wall[...], rounded, preferred_element_type=jnp.float32)
            gz = jnp.dot(rounded, span[...], preferred_element_type=jnp.float32)
            out.append(-(vx * (after(c) - before(c)) + vel[1] * gy + vel[2] * gz))
        return out

    plane = lambda i: lambda c: order[i][0][c, order[i][1]]
    for i in range(1, 5):
        f0 = rate(plane(i - 1), plane(i), plane(i + 1))
        for c in range(3):
            mid[c, i - 1] = plane(i)(c) + STEP * f0[c]
            if i in (2, 3):
                b_ref[c, one(i - 2)] = f0[c] * (-0.5 * STEP)
    for i in (1, 2):
        f1 = rate(lambda c: mid[c, i - 1], lambda c: mid[c, i], lambda c: mid[c, i + 1])
        for c in range(3):
            at = one(i - 1)
            u1 = mid[c, i]
            a_ref[c, at] = u1 + STEP * f1[c]
            b_ref[c, at] = b_ref[c, at] + (0.5 * STEP) * f1[c] + first * u1


def evaluate(flags, near, own, far, wall, span, flow):
    shape = jax.ShapeDtypeStruct(own.shape, own.dtype)
    vmem = pl.BlockSpec(memory_space=pltpu.VMEM)
    parts, planes, ys, zs = own.shape
    return pl.pallas_call(
        advance,
        out_shape=(shape, shape),
        in_specs=[pl.BlockSpec(memory_space=pltpu.SMEM)] + [vmem] * 6,
        out_specs=(vmem, vmem),
        scratch_shapes=[pltpu.VMEM((parts, planes + 2, ys, zs), jnp.float32)],
        cost_estimate=pl.CostEstimate(flops=6 * 6 * 2 * ys * ys * zs, bytes_accessed=5 * own.size * 4, transcendentals=0),
        name="advance",
    )(flags, near, own, far, wall, span, flow)


def local(ways, start_states, wall_normal, spanwise, base_flow):
    home = start_states[0]
    slice_at, slab_at = lax.axis_index("tm"), lax.axis_index("space")
    core, chip = slice_at % 2, slab_at % 2
    mover = core != chip
    first = (slice_at // 2 == 0) & (chip == 0)
    flags = jnp.stack([core, first.astype(core.dtype)]).astype(jnp.int32)
    flow = jnp.broadcast_to(base_flow[:, :, None], base_flow.shape + home.shape[-1:])
    send = lambda what, way: lax.ppermute(what, AXES, ways[way])
    step = functools.partial(evaluate, flags, wall=wall_normal, span=spanwise, flow=flow)

    swapped = send(home, "swap")
    far_in = send(home, "far_in")
    near_in = send(home, "near_in")
    far_out = send(swapped, "far_out")
    near_out = send(swapped, "near_out")
    a_move, b_move = step(near_in, swapped, far_in)
    back = send(b_move, "swap")
    next_move = send(a_move, "next_move")
    a_stay, b_stay = step(near_out, home, far_out)
    next_stay = send(a_stay, "next_stay")
    return (jnp.where(mover, back, b_stay) + (next_move + next_stay))[None]


def solution(mesh):
    placed = (P("tm", None, "space", None, None), P(), P(), P())
    ways = routes(mesh.shape["tm"], mesh.shape["space"])
    return jax.shard_map(
        functools.partial(local, ways),
        mesh=mesh,
        in_specs=placed,
        out_specs=P("tm", None, "space", None, None),
        check_vma=False,
    )
```

```python
import functools

import jax
import jax.numpy as jnp
from jax import lax
from jax.experimental import pallas as pl
from jax.experimental.pallas import tpu as pltpu
from jax.sharding import PartitionSpec as P


AXES = ("tm", "space")
STEP = 0.2
EARLY = 2


def routes(slices, slabs):
    at = lambda s, p: s * slabs + p % slabs
    cells = [(k, x, l) for k in range(slices // 2) for x in range(slabs // 2) for l in range(2)]
    side = lambda l: 1 - 2 * l
    stay = lambda k, x, l: at(2 * k + l, 2 * x + l)
    move = lambda k, x, l: at(2 * k + 1 - l, 2 * x + l)
    return {
        "swap": [(move(k, x, l), move(k, x, 1 - l)) for k, x, l in cells],
        "near_in": [(stay(k, x, l), move(k, x, l)) for k, x, l in cells],
        "far_in": [(stay(k, x + side(l), l), move(k, x, l)) for k, x, l in cells],
        "near_out": [(move(k, x, l), stay(k, x, l)) for k, x, l in cells],
        "far_out": [(move(k, x, l), stay(k, x + side(l), l)) for k, x, l in cells],
        "next_move": [
            (move(k, x, l), at(2 * k + l + 1, 2 * x + 1 - l)) for k, x, l in cells if 2 * k + l + 1 < slices
        ],
        "next_stay": [(stay(k, x, l), at(2 * k + l + 1, 2 * x + l)) for k, x, l in cells if 2 * k + l + 1 < slices],
    }


def advance(sizes, *refs):
    pieces, refs = refs[: sum(map(len, sizes))], refs[sum(map(len, sizes)) :]
    wall, span, base, a_early, a_late, b_out, mid, a_mid, b_mid, flow, out_sems = refs
    slice_at, slab_at = lax.axis_index(AXES[0]), lax.axis_index(AXES[1])
    low = slice_at % 2
    leading = (slice_at < 2) & (slab_at % 2 == 0)
    half = jnp.where(low == 1, 0.5, -0.5).astype(jnp.float32)
    slot = lambda i: jnp.where(low == 1, i % 2, 1 - i % 2)

    plane = []
    for i in range(6):
        first_piece = sum(len(sizes[k]) for k in range(i // 2))
        plane.append(
            [
                (pieces[first_piece + n], c)
                for n, size in enumerate(sizes[i // 2])
                for c in range(size)
            ]
        )

    def load(i):
        return lambda c: plane[i][c][0][plane[i][c][1], slot(i)]

    for c in range(3):
        rows = jnp.broadcast_to(base[c : c + 1], (8, base.shape[1]))
        flow[c] = jnp.broadcast_to(rows.T[:, :1], flow.shape[1:])

    def slope(before, here, after):
        fields = [here(c) for c in range(3)]
        vx, vy, vz = [jnp.concatenate([flow[c]] * 2, axis=1) + fields[c] for c in range(3)]
        vx = vx * half
        for c in range(3):
            rounded = fields[c].astype(jnp.bfloat16)
            gy = jnp.dot(wall[...], rounded, preferred_element_type=jnp.float32)
            gz = jnp.dot(rounded, span[...], preferred_element_type=jnp.float32)
            yield fields[c], vx * (after(c) - before(c)) + vy * gy + vz * gz

    def inner(i):
        for c, (u0, g0) in enumerate(slope(load(i - 1), load(i), load(i + 1))):
            mid[c, i - 1] = u0 - STEP * g0
            if i in (2, 3):
                b_mid[c, i - 2] = g0 * (0.5 * STEP)

    def outer(i):
        for c, (u1, g1) in enumerate(slope(*[lambda c, k=k: mid[c, k] for k in (i - 2, i - 1, i)])):
            a_mid[c, i - 2] = u1 - STEP * g1
            b_mid[c, i - 2] = b_mid[c, i - 2] - (0.5 * STEP) * g1

        @pl.when(leading)
        def _():
            b_mid[:, i - 2] = b_mid[:, i - 2] + mid[:, i - 1]

        place = i - 2, slot(i)
        sends = [
            pltpu.make_async_copy(value.at[:, place[0]], out.at[:, place[1]], out_sems.at[n, i - 2])
            for n, (value, out) in enumerate(
                ((b_mid, b_out), (a_mid.at[:EARLY], a_early), (a_mid.at[EARLY:], a_late))
            )
        ]
        for send in sends:
            send.start()
        return sends

    inner(1)
    inner(2)
    inner(3)
    sends = outer(2)
    inner(4)
    sends += outer(3)
    for send in sends:
        send.wait()


def evaluate(slabs, wall, span, base):
    sizes = [[piece.shape[0] for piece in slab] for slab in slabs]
    pieces = [piece for slab in slabs for piece in slab]
    planes, ys, zs = pieces[0].shape[1:]
    shape = lambda n: jax.ShapeDtypeStruct((n, planes, ys, zs), jnp.float32)
    vmem = pl.BlockSpec(memory_space=pltpu.VMEM)
    any_space = pl.BlockSpec(memory_space=pl.ANY)
    block = lambda n: pltpu.VMEM((3, n, ys, zs), jnp.float32)
    return pl.pallas_call(
        functools.partial(advance, sizes),
        out_shape=(shape(EARLY), shape(3 - EARLY), shape(3)),
        in_specs=[vmem] * (len(pieces) + 3),
        out_specs=(any_space,) * 3,
        scratch_shapes=[
            block(4),
            block(2),
            block(2),
            pltpu.VMEM((3, ys, zs // 2), jnp.float32),
            pltpu.SemaphoreType.DMA((3, 2)),
        ],
        compiler_params=pltpu.CompilerParams(vmem_limit_bytes=12 * 2**20),
        cost_estimate=pl.CostEstimate(flops=36 * 2 * ys * ys * zs, bytes_accessed=30 * ys * zs * 4, transcendentals=0),
        name="advance",
    )(*pieces, wall, span, base)


def local(ways, start_states, wall_normal, spanwise, base_flow):
    home = start_states[0]
    mover = lax.axis_index("tm") % 2 != lax.axis_index("space") % 2
    step = functools.partial(evaluate, wall=wall_normal, span=spanwise, base=base_flow)

    def send(what, way):
        return lax.ppermute(what, AXES, ways[way])

    far_in = send(home, "far_in")
    own_early = send(home[:EARLY], "swap")
    own_late = send(home[EARLY:], "swap")
    near_in = send(home, "near_in")
    far_early = send(own_early, "far_out")
    near_early = send(own_early, "near_out")
    move_early, move_late, b_move = step([[near_in], [own_early, own_late], [far_in]])
    back = send(b_move, "swap")
    far_late = send(own_late, "far_out")
    move_early = send(move_early, "next_move")
    move_late = send(move_late, "next_move")
    near_late = send(own_late, "near_out")
    stay_early, stay_late, b_stay = step([[near_early, near_late], [home], [far_early, far_late]])
    stay_early = send(stay_early, "next_stay")
    stay_late = send(stay_late, "next_stay")
    result = jnp.where(mover, back, b_stay)
    result = result.at[:EARLY].add(jnp.where(mover, stay_early, move_early))
    result = result.at[EARLY:].add(jnp.where(mover, stay_late, move_late))
    return result[None]


def solution(mesh):
    placed = (P("tm", None, "space", None, None), P(), P(), P())
    ways = routes(mesh.shape["tm"], mesh.shape["space"])
    return jax.shard_map(
        functools.partial(local, ways),
        mesh=mesh,
        in_specs=placed,
        out_specs=P("tm", None, "space", None, None),
        check_vma=False,
    )
```

```python
import functools

import jax
import jax.numpy as jnp
from jax import lax
from jax.experimental import pallas as pl
from jax.experimental.pallas import tpu as pltpu
from jax.sharding import PartitionSpec as P


AXES = ("tm", "space")
STEP = 0.2
EARLY = 2


def routes(slices, slabs):
    at = lambda s, p: s * slabs + p % slabs
    cells = [(k, x, l) for k in range(slices // 2) for x in range(slabs // 2) for l in range(2)]
    side = lambda l: 1 - 2 * l
    stay = lambda k, x, l: at(2 * k + l, 2 * x + l)
    move = lambda k, x, l: at(2 * k + 1 - l, 2 * x + l)
    return {
        "swap": [(move(k, x, l), move(k, x, 1 - l)) for k, x, l in cells],
        "near_in": [(stay(k, x, l), move(k, x, l)) for k, x, l in cells],
        "far_in": [(stay(k, x + side(l), l), move(k, x, l)) for k, x, l in cells],
        "near_out": [(move(k, x, l), stay(k, x, l)) for k, x, l in cells],
        "far_out": [(move(k, x, l), stay(k, x + side(l), l)) for k, x, l in cells],
        "next_move": [
            (move(k, x, l), at(2 * k + l + 1, 2 * x + 1 - l)) for k, x, l in cells if 2 * k + l + 1 < slices
        ],
        "next_stay": [(stay(k, x, l), at(2 * k + l + 1, 2 * x + l)) for k, x, l in cells if 2 * k + l + 1 < slices],
    }


def advance(sizes, which, movers, *refs):
    mover = lax.axis_index(AXES[0]) % 2 != lax.axis_index(AXES[1]) % 2
    pl.when(mover == movers)(lambda: advance_plane(sizes, which, *refs))


def advance_plane(sizes, which, *refs):
    pieces, refs = refs[: sum(map(len, sizes))], refs[sum(map(len, sizes)) :]
    wall, span, base, a_out, b_out, mid, flow = refs
    slice_at, slab_at = lax.axis_index(AXES[0]), lax.axis_index(AXES[1])
    low = slice_at % 2
    lead = jnp.where((slice_at < 2) & (slab_at % 2 == 0), 1.0, 0.0).astype(jnp.float32)
    half = jnp.where(low == 1, 0.5, -0.5).astype(jnp.float32)

    def load(i):
        first_piece = sum(map(len, sizes[: i // 2]))
        entries = [(first_piece + n, c) for n, size in enumerate(sizes[i // 2]) for c in range(size)]
        slot = jnp.where(low == 1, i % 2, 1 - i % 2)
        return lambda c: pieces[entries[c][0]][entries[c][1], slot]

    for c in range(3):
        rows = jnp.broadcast_to(base[c : c + 1], (8, base.shape[1]))
        flow[c] = jnp.broadcast_to(rows.T[:, :1], flow.shape[1:])

    def slope(before, here, after):
        fields = [here(c) for c in range(3)]
        vx, vy, vz = [jnp.concatenate([flow[c]] * 2, axis=1) + fields[c] for c in range(3)]
        vx = vx * half
        for c in range(3):
            rounded = fields[c].astype(jnp.bfloat16)
            gy = jnp.dot(wall[...], rounded, preferred_element_type=jnp.float32)
            gz = jnp.dot(rounded, span[...], preferred_element_type=jnp.float32)
            yield fields[c], vx * (after(c) - before(c)) + vy * gy + vz * gz

    for n in range(3):
        i = which + n + 1
        for c, (u0, g0) in enumerate(slope(load(i - 1), load(i), load(i + 1))):
            u1 = u0 - STEP * g0
            mid[c, n] = u1
            if n == 1:
                b_out[c] = g0 * (0.5 * STEP) + lead * u1
    for c, (u1, g1) in enumerate(slope(*[lambda c, n=n: mid[c, n] for n in range(3)])):
        b_out[c] = b_out[c] - (0.5 * STEP) * g1
        a_out[c] = u1 - STEP * g1


def evaluate(slabs, which, movers, wall, span, base):
    sizes = [[piece.shape[0] for piece in slab] for slab in slabs]
    pieces = [piece for slab in slabs for piece in slab]
    ys, zs = pieces[0].shape[2:]
    shape = jax.ShapeDtypeStruct((3, ys, zs), jnp.float32)
    vmem = pl.BlockSpec(memory_space=pltpu.VMEM)
    return pl.pallas_call(
        functools.partial(advance, sizes, which, movers),
        out_shape=(shape, shape),
        in_specs=[vmem] * (len(pieces) + 3),
        out_specs=(vmem, vmem),
        scratch_shapes=[
            pltpu.VMEM((3, 3, ys, zs), jnp.float32),
            pltpu.VMEM((3, ys, zs // 2), jnp.float32),
        ],
        compiler_params=pltpu.CompilerParams(vmem_limit_bytes=12 * 2**20),
        cost_estimate=pl.CostEstimate(flops=24 * 2 * ys * ys * zs, bytes_accessed=21 * ys * zs * 4, transcendentals=0),
        name="advance",
    )(*pieces, wall, span, base)


def finish(which, *refs):
    back, b_stay, stay, move, out, first, second, sems = refs[-8:]
    slice_at, slab_at = lax.axis_index(AXES[0]), lax.axis_index(AXES[1])
    mover = slice_at % 2 != slab_at % 2
    slot = jnp.where(slab_at % 2 == 1, which, 1 - which)
    parts = range(first.shape[0])
    copies = lambda one, two: [
        (
            pltpu.make_async_copy(one.at[c], first.at[c], sems.at[0, c]),
            pltpu.make_async_copy(two.at[c], second.at[c], sems.at[1, c]),
        )
        for c in parts
    ]

    def start(one, two):
        for pair in copies(one, two):
            for copy in pair:
                copy.start()

    pl.when(mover)(lambda: start(back, stay))
    pl.when(jnp.logical_not(mover))(lambda: start(b_stay, move))
    writes = []
    for c, pair in enumerate(copies(back, stay)):
        for copy in pair:
            copy.wait()
        first[c] = first[c] + second[c]
        writes.append(pltpu.make_async_copy(first.at[c], out.at[c, slot], sems.at[2, c]))
        writes[-1].start()
    for write in writes:
        write.wait()


def combine(result, which, *parts):
    shape = parts[0].shape
    any_space = pl.BlockSpec(memory_space=pl.ANY)
    operands = parts if result is None else (result, *parts)
    return pl.pallas_call(
        functools.partial(finish, which),
        out_shape=jax.ShapeDtypeStruct((shape[0], 2, *shape[1:]), jnp.float32),
        in_specs=[any_space] * len(operands),
        out_specs=any_space,
        input_output_aliases={} if result is None else {0: 0},
        scratch_shapes=[
            pltpu.VMEM(shape, jnp.float32),
            pltpu.VMEM(shape, jnp.float32),
            pltpu.SemaphoreType.DMA((3, shape[0])),
        ],
        compiler_params=pltpu.CompilerParams(vmem_limit_bytes=4 * 2**20),
        name="finish",
    )(*operands)


def local(ways, start_states, wall_normal, spanwise, base_flow):
    home = start_states[0]
    step = functools.partial(evaluate, wall=wall_normal, span=spanwise, base=base_flow)

    def send(what, way):
        return lax.ppermute(what, AXES, ways[way])

    far_in = send(home, "far_in")
    own_early = send(home[:EARLY], "swap")
    own_late = send(home[EARLY:], "swap")
    near_in = send(home, "near_in")
    far_early = send(own_early, "far_out")
    near_early = send(own_early, "near_out")
    slabs = [[near_in], [own_early, own_late], [far_in]]
    a_move_0, b_move_0 = step(slabs, 0, True)
    back_0 = send(b_move_0, "swap")
    move_0 = send(a_move_0, "next_move")
    far_late = send(own_late, "far_out")
    near_late = send(own_late, "near_out")
    a_move_1, b_move_1 = step(slabs, 1, True)
    back_1 = send(b_move_1, "swap")
    move_1 = send(a_move_1, "next_move")
    slabs = [[near_early, near_late], [home], [far_early, far_late]]
    a_stay_0, b_stay_0 = step(slabs, 0, False)
    stay_0 = send(a_stay_0, "next_stay")
    a_stay_1, b_stay_1 = step(slabs, 1, False)
    stay_1 = send(a_stay_1, "next_stay")
    result = combine(None, 0, back_0, b_stay_0, stay_0, move_0)
    return combine(result, 1, back_1, b_stay_1, stay_1, move_1)[None]


def solution(mesh):
    placed = (P("tm", None, "space", None, None), P(), P(), P())
    ways = routes(mesh.shape["tm"], mesh.shape["space"])
    return jax.shard_map(
        functools.partial(local, ways),
        mesh=mesh,
        in_specs=placed,
        out_specs=P("tm", None, "space", None, None),
        check_vma=False,
    )
```
